32 devices in a mesh: gz: 2 (over core), gx: 4 (over z), gy: 4 (over y, x).
Axes of the slice: x: 2, y: 2, z: 4, core: 2. Of those that a mesh axis runs over, the one named last changes fastest.
Arguments:
- pair_repr: bfloat16 [8, 384, 384, 128], P('gz', 'gx', 'gy'), may hold values from -9 to 9
- seq_lengths: int32 [8], replicated, may hold values from 96 to 384
- weight_in: bfloat16 [128, 640], replicated, may hold values from -0.5 to 0.5
- weight_out: bfloat16 [128, 128], replicated, may hold values from -0.5 to 0.5
Outputs:
- updated: bfloat16 [8, 384, 384, 128], P('gz', 'gx', 'gy')
- magnitude: float32 [], replicated
The draws below stay inside these ranges and needn't reach their ends.
All inputs are finite; a program needn't handle non-finite values.
Results may differ from the reference program's by a relative error of at most 0.0034.
Values may be sent and summed in bfloat16 or wider, within the bound.
A program may use at most 384 MiB of HBM per device.

```python
import math
import jax
import jax.numpy as jnp
from jax import lax

C = 128
CH = 128
N = 384
BATCH = 8


def draw_pair_repr(key, part):
    split_keys = jax.random.split(jax.random.fold_in(key, 17), 3)
    row_ramp = 0.5 + jnp.arange(N, dtype=jnp.float32) / N
    row_scale = jnp.exp(jax.random.uniform(split_keys[1], (BATCH, N, 1, 1), jnp.float32, math.log(0.7), math.log(1.4)))
    col_scale = jnp.exp(jax.random.uniform(split_keys[2], (BATCH, 1, N, 1), jnp.float32, math.log(0.7), math.log(1.4)))
    base_values = jnp.clip(jax.random.normal(split_keys[0], (BATCH, N, N, C), jnp.float32), -3.0, 3.0)
    values = base_values * row_ramp[None, :, None, None] * row_scale * col_scale
    return values.astype(jnp.bfloat16)


def with_ends(array, key, least, top_value):
    longest = array.shape.index(max(array.shape))
    spots = []
    for shift in (0, 1):
        where = [jax.random.randint(jax.random.fold_in(key, axis), (), 0, length) for axis, length in enumerate(array.shape)]
        where[longest] = (where[longest] + shift) % array.shape[longest]
        spots.append(tuple(where))
    return array.at[spots[0]].set(least).at[spots[1]].set(top_value)


def noise(rng, extent, scale, most, held_as=jnp.bfloat16):
    array = scale * jax.random.normal(rng, extent, jnp.float32)
    return jnp.clip(array, min=-most, max=most).astype(held_as)


def setup_inputs(seed: int = 0) -> dict:
    seeds = jax.random.split(jax.random.key(seed), 5)
    pair_repr = draw_pair_repr(jax.random.fold_in(seeds[4], 71), 0)
    seq_lengths = with_ends(jax.random.randint(seeds[1], (BATCH,), N // 4, N + 1), jax.random.fold_in(seeds[1], 1), N // 4, N).astype(jnp.int32)
    weight_in = noise(seeds[2], (C, 4 * CH + C), C ** -0.5, 0.5)
    weight_out = noise(seeds[3], (CH, C), CH ** -0.5, 0.5)
    return dict(pair_repr=pair_repr, seq_lengths=seq_lengths, weight_in=weight_in, weight_out=weight_out)


def layer_norm(values):
    mean_value = lax.optimization_barrier(jnp.mean(values, axis=-1, keepdims=True))
    centered = values - mean_value
    variance = lax.optimization_barrier(jnp.mean(centered * centered, axis=-1, keepdims=True))
    return centered * lax.rsqrt(variance + 1e-05)

def reference(pair_repr, seq_lengths, weight_in, weight_out):

    def one_tensor(inputs):
        pair_one, length_one = inputs
        positions = jnp.arange(N, dtype=jnp.int32)
        row_live = (positions < length_one).astype(jnp.float32)
        pair_mask = (row_live[:, None] * row_live[None, :])[:, :, None]
        normed = layer_norm(pair_one.astype(jnp.float32)).astype(jnp.bfloat16)
        proj = jnp.dot(normed.reshape(N * N, C), weight_in, preferred_element_type=jnp.float32).reshape(N, N, 4 * CH + C)
        left_proj = (pair_mask * jax.nn.sigmoid(proj[..., CH:2 * CH]) * proj[..., :CH]).astype(jnp.bfloat16)
        right_proj = (pair_mask * jax.nn.sigmoid(proj[..., 3 * CH:4 * CH]) * proj[..., 2 * CH:3 * CH]).astype(jnp.bfloat16)
        gate_values = jax.nn.sigmoid(proj[..., 4 * CH:])
        triangle = jnp.einsum('kic,kjc->ijc', left_proj.astype(jnp.float32), right_proj.astype(jnp.float32), precision=lax.Precision.HIGHEST)
        tri_normed = layer_norm(triangle).astype(jnp.bfloat16)
        projected = jnp.dot(tri_normed.reshape(N * N, CH), weight_out, preferred_element_type=jnp.float32).reshape(N, N, C)
        update = pair_mask * gate_values * projected
        return (pair_one.astype(jnp.float32) + update).astype(jnp.bfloat16)
    updated = lax.map(one_tensor, (pair_repr, seq_lengths))
    entry_count = float(BATCH * N * N * C)
    magnitude = jnp.sum(jnp.abs(updated.astype(jnp.float32))) / entry_count
    return (updated, magnitude)
```

```python
import jax
import jax.numpy as jnp
from jax import lax
from jax.sharding import PartitionSpec as P

CHUNKS = 3


def layer_norm(values):
    mean_value = jnp.mean(values, axis=-1, keepdims=True)
    centered = values - mean_value
    variance = jnp.mean(centered * centered, axis=-1, keepdims=True)
    return centered * lax.rsqrt(variance + 1e-05)


def project(normed, weight):
    return jnp.einsum("ijc,cd->ijd", normed, weight, preferred_element_type=jnp.float32)


def rehomed(pair_repr, seq_lengths, weight_in, weight_out):
    batch_dev, row_count, col_count, channels = pair_repr.shape
    hidden = weight_out.shape[0]
    ring = batch_dev
    me = lax.axis_index("gx")
    row_first = me * row_count
    col_first = lax.axis_index("gy") * col_count
    my_lengths = lax.dynamic_slice_in_dim(seq_lengths, lax.axis_index("gz") * batch_dev, batch_dev)
    my_length = lax.dynamic_index_in_dim(my_lengths, me, 0, keepdims=False)
    col_at = col_first + jnp.arange(col_count, dtype=jnp.int32)
    row_local = jnp.arange(row_count, dtype=jnp.int32)
    width = col_count // CHUNKS
    tall = row_count // CHUNKS

    def shift(value, step):
        if step == 0:
            return value
        return lax.ppermute(value, "gx", [(i, (i + step) % ring) for i in range(ring)])

    def gated(normed, first, mask):
        proj = project(normed, weight_in[:, first : first + 2 * hidden])
        return (mask * jax.nn.sigmoid(proj[..., hidden:]) * proj[..., :hidden]).astype(
            jnp.bfloat16
        )

    to = [lax.rem(me + s, ring) for s in range(ring)]
    source = [lax.rem(me + ring - s, ring) for s in range(ring)]
    outgoing = [lax.dynamic_index_in_dim(pair_repr, to[s], 0, keepdims=False) for s in range(ring)]
    k_at = jnp.concatenate([source[s] * row_count + row_local for s in range(ring)])
    k_live = (k_at < my_length).astype(jnp.float32)

    lefts, rights = [], []
    for t in range(CHUNKS):
        cols = slice(t * width, (t + 1) * width)
        got = [shift(outgoing[s][:, cols], s) for s in range(ring)]
        mine = jnp.concatenate(got, axis=0)
        normed = layer_norm(mine.astype(jnp.float32)).astype(jnp.bfloat16)
        live = (col_at[cols] < my_length).astype(jnp.float32)
        mask = k_live[:, None, None] * live[None, :, None]
        left = gated(normed, 0, mask)
        lefts.append(lax.all_gather(left, "gy", axis=0))
        rights.append(gated(normed, 2 * hidden, mask))
    right = jnp.concatenate(rights, axis=1)

    updated = jnp.zeros_like(pair_repr)
    total = jnp.float32(0)
    for t in range(CHUNKS):
        rows = slice(t * tall, (t + 1) * tall)
        triangle = jnp.einsum("gkic,kjc->gijc", lefts[t], right, preferred_element_type=jnp.float32)
        tri_normed = layer_norm(triangle).astype(jnp.bfloat16)
        for s in range(ring):
            home = shift(lax.dynamic_index_in_dim(tri_normed, to[s], 0, keepdims=False), s)
            b = source[s]
            own = lax.dynamic_slice(
                pair_repr, (b, t * tall, 0, 0), (1, tall, col_count, channels)
            )[0].astype(jnp.float32)
            length = lax.dynamic_index_in_dim(my_lengths, b, 0, keepdims=False)
            row_live = (row_first + row_local[rows] < length).astype(jnp.float32)
            col_live = (col_at < length).astype(jnp.float32)
            mask = row_live[:, None, None] * col_live[None, :, None]
            gate_values = jax.nn.sigmoid(
                project(layer_norm(own).astype(jnp.bfloat16), weight_in[:, 4 * hidden :])
            )
            one = (own + mask * gate_values * project(home, weight_out)).astype(jnp.bfloat16)
            updated = lax.dynamic_update_slice(updated, one[None], (b, t * tall, 0, 0))
            total = total + jnp.sum(jnp.abs(one.astype(jnp.float32)))
    mag_total = lax.psum(total, ("gz", "gx", "gy"))
    entry_count = batch_dev * lax.axis_size("gz") * row_count * ring * col_count * lax.axis_size("gy") * channels
    return (updated, mag_total / float(entry_count))


def gathered_columns(pair_repr, seq_lengths, weight_in, weight_out):
    batch_dev, row_count, col_count, channels = pair_repr.shape
    hidden = weight_out.shape[0]
    row_first = lax.axis_index("gx") * row_count
    col_first = lax.axis_index("gy") * col_count
    my_lengths = lax.dynamic_slice_in_dim(seq_lengths, lax.axis_index("gz") * batch_dev, batch_dev)
    row_at = row_first + jnp.arange(row_count, dtype=jnp.int32)
    col_at = col_first + jnp.arange(col_count, dtype=jnp.int32)

    def gated(normed, first, mask):
        part = weight_in[:, first : first + 2 * hidden]
        proj = jnp.einsum("ijc,cd->ijd", normed, part, preferred_element_type=jnp.float32)
        return (mask * jax.nn.sigmoid(proj[..., hidden:]) * proj[..., :hidden]).astype(
            jnp.bfloat16
        )

    masks, normed, gathered, shares = [], [], [], []
    for b in range(batch_dev):
        row_live = (row_at < my_lengths[b]).astype(jnp.float32)
        col_live = (col_at < my_lengths[b]).astype(jnp.float32)
        masks.append(row_live[:, None, None] * col_live[None, :, None])
        normed.append(layer_norm(pair_repr[b].astype(jnp.float32)).astype(jnp.bfloat16))
        left = gated(normed[b], 0, masks[b])
        gathered.append(lax.all_gather(left, "gy", axis=1, tiled=True))
    for b in range(batch_dev):
        right = gated(normed[b], 2 * hidden, masks[b])
        partial = jnp.einsum(
            "kic,kjc->ijc", gathered[b], right, preferred_element_type=jnp.float32
        ).astype(jnp.bfloat16)
        shares.append(lax.psum_scatter(partial, "gx", scatter_dimension=0, tiled=True))
    outs, total = [], jnp.float32(0)
    for b in range(batch_dev):
        gate_values = jax.nn.sigmoid(
            jnp.einsum(
                "ijc,cd->ijd", normed[b], weight_in[:, 4 * hidden :],
                preferred_element_type=jnp.float32,
            )
        )
        tri_normed = layer_norm(shares[b].astype(jnp.float32)).astype(jnp.bfloat16)
        projected = jnp.einsum(
            "ijc,cd->ijd", tri_normed, weight_out, preferred_element_type=jnp.float32
        )
        update = masks[b] * gate_values * projected
        one = (pair_repr[b].astype(jnp.float32) + update).astype(jnp.bfloat16)
        outs.append(one)
        total = total + jnp.sum(jnp.abs(one.astype(jnp.float32)))
    updated = jnp.stack(outs)
    mag_total = lax.psum(total, ("gz", "gx", "gy"))
    entry_count = (
        batch_dev
        * lax.axis_size("gz")
        * row_count
        * lax.axis_size("gx")
        * col_count
        * lax.axis_size("gy")
        * channels
    )
    magnitude = mag_total / float(entry_count)
    return (updated, magnitude)


def per_device(pair_repr, seq_lengths, weight_in, weight_out):
    batch_dev, row_count, col_count, _ = pair_repr.shape
    fits = row_count % CHUNKS == 0 and col_count % CHUNKS == 0
    if fits and lax.axis_size("gx") == batch_dev and lax.axis_size("gy") == batch_dev:
        return rehomed(pair_repr, seq_lengths, weight_in, weight_out)
    return gathered_columns(pair_repr, seq_lengths, weight_in, weight_out)


def solution(mesh):
    return jax.shard_map(
        per_device,
        mesh=mesh,
        in_specs=(P("gz", "gx", "gy", None), P(), P(), P()),
        out_specs=(P("gz", "gx", "gy", None), P()),
        check_vma=False,
    )
```

```python
import functools

import jax
import jax.numpy as jnp
from jax import lax
from jax.experimental import pallas as pl
from jax.experimental.pallas import tpu as pltpu
from jax.sharding import PartitionSpec as P

WIDTH = 16
UNROLL = 2
LANES = 128
EPS = 1e-05


def layer_norm(values):
    mean_value = jnp.mean(values, axis=-1, keepdims=True)
    centered = values - mean_value
    variance = jnp.mean(centered * centered, axis=-1, keepdims=True)
    return centered * lax.rsqrt(variance + EPS)


def contract_last(a, b):
    return lax.dot_general(a, b, (((1,), (1,)), ((), ())), preferred_element_type=jnp.float32)


def meet(axes):
    barrier = pltpu.get_barrier_semaphore()
    for axis, size in axes:
        me = lax.axis_index(axis)
        for s in range(1, size):
            pl.semaphore_signal(
                barrier, inc=1, device_id={axis: lax.rem(me + s, size)},
                device_id_type=pl.DeviceIdType.MESH,
            )
    pl.semaphore_wait(barrier, sum(size - 1 for _, size in axes))


def remote(src, dst, send, recv, axis, target):
    return pltpu.make_async_remote_copy(
        src_ref=src, dst_ref=dst, send_sem=send, recv_sem=recv,
        device_id={axis: target}, device_id_type=pl.DeviceIdType.MESH,
    )


def enter_kernel(
    ring, pair_ref, weight_ref, mask_ref, sides_ref, got_ref,
    block, stage, ready, load_sem, z_send, z_recv, y_send, y_recv, own_sem,
):
    me, col = lax.axis_index("gx"), lax.axis_index("gy")
    cols, rows = pair_ref.shape[1], pair_ref.shape[2]
    hidden = weight_ref.shape[0] // 4
    quarter = hidden // ring
    steps = cols // WIDTH
    deep = ring * rows
    meet((("gx", ring), ("gy", ring)))

    def inbound(t, s):
        target = jnp.bitwise_xor(me, s)
        part = pl.ds(pl.multiple_of(t * WIDTH, WIDTH), WIDTH)
        return remote(
            pair_ref.at[target, part], got_ref.at[s - 1, part],
            z_send.at[t, s - 1], z_recv.at[t, s - 1], "gx", target,
        )

    def outbound(t, s):
        target = jnp.bitwise_xor(col, s)
        return remote(
            ready.at[lax.rem(t, 2), target], sides_ref.at[t, col],
            y_send.at[t, s - 1], y_recv.at[t, s - 1], "gy", target,
        )

    def own(t):
        return pltpu.make_async_copy(
            ready.at[lax.rem(t, 2), col], sides_ref.at[t, col], own_sem.at[t]
        )

    for t in range(steps):
        for s in range(1, ring):
            inbound(t, s).start()

    def drain(t):
        for s in range(1, ring):
            outbound(t, s).wait_send()
        own(t).wait()

    def step(t, carry):
        for s in range(1, ring):
            inbound(t, s).wait_recv()
        part = pl.ds(pl.multiple_of(t * WIDTH, WIDTH), WIDTH)
        loads = []
        for s in range(ring):
            src = pair_ref.at[me, part] if s == 0 else got_ref.at[s - 1, part]
            loads.append(
                pltpu.make_async_copy(src, block.at[:, pl.ds(s * rows, rows)], load_sem.at[s])
            )
            loads[-1].start()
        for load in loads:
            load.wait()

        def column(i, carry):
            normed = layer_norm(block[i].astype(jnp.float32)).astype(jnp.bfloat16)
            proj = contract_last(weight_ref[...], normed)
            live = mask_ref[pl.ds(t * WIDTH + i, 1), :]
            for side in range(2):
                first = 2 * side * hidden
                value = proj[first : first + hidden]
                gate = proj[first + hidden : first + 2 * hidden]
                out = live * jax.nn.sigmoid(gate) * value
                for l in range(deep // LANES):
                    stage[l, pl.ds(side * hidden * WIDTH + i, hidden, stride=WIDTH), :] = out[
                        :, l * LANES : (l + 1) * LANES
                    ]
            return carry

        lax.fori_loop(0, WIDTH, column, 0, unroll=UNROLL)

        @pl.when(t >= 2)
        def _():
            drain(t - 2)

        slot = lax.rem(t, 2)
        for side in range(2):
            for q in range(ring):
                first = (side * hidden + q * quarter) * WIDTH
                for l in range(deep // LANES):
                    ready[slot, q, side, :, :, l * LANES : (l + 1) * LANES] = (
                        stage[l, first : first + quarter * WIDTH, :]
                        .reshape(quarter, WIDTH, LANES)
                        .astype(jnp.bfloat16)
                    )
        for s in range(1, ring):
            outbound(t, s).start()
        own(t).start()
        return carry

    lax.fori_loop(0, steps, step, 0)
    for t in range(max(steps - 2, 0), steps):
        drain(t)
    for t in range(steps):
        for s in range(1, ring):
            inbound(t, s).wait_send()
            outbound(t, s).wait_recv()


def leave_kernel(
    ring, pairs, sides_ref, pair_ref, gate_ref, out_ref, live_ref, col_ref,
    updated_ref, total_ref, tri_ref, home_ref,
    left, right, product, part_ref, stage, normed_ref, home, pair, result, sums, boxes,
    load_sem, y_send, y_recv, y_own, z_send, z_recv, z_own, keep_sem, sum_send, sum_recv, side_sem,
):
    me, col = lax.axis_index("gx"), lax.axis_index("gy")
    cols, rows, channels = pair_ref.shape[1:]
    quarter = sides_ref.shape[3]
    hidden = ring * quarter
    steps = cols // WIDTH
    wide = ring * rows
    axes = (("gx", ring), ("gy", ring), ("gz", pairs))
    meet(axes)

    def part(t):
        return pl.ds(pl.multiple_of(t * WIDTH, WIDTH), WIDTH)

    def across(t, s):
        target = jnp.bitwise_xor(col, s)
        return remote(
            product.at[lax.rem(t, 2), target], tri_ref.at[t, col],
            y_send.at[t, s - 1], y_recv.at[t, s - 1], "gy", target,
        )

    def across_own(t):
        return pltpu.make_async_copy(
            product.at[lax.rem(t, 2), col], tri_ref.at[t, col], y_own.at[t]
        )

    def homeward(t, s):
        target = jnp.bitwise_xor(me, s)
        return remote(
            normed_ref.at[lax.rem(t, 2), target], home_ref.at[me, part(t)],
            z_send.at[t, s - 1], z_recv.at[t, s - 1], "gx", target,
        )

    def homeward_own(t):
        return pltpu.make_async_copy(
            normed_ref.at[lax.rem(t, 2), me], home_ref.at[me, part(t)], z_own.at[t]
        )

    def keep(t):
        return pltpu.make_async_copy(result, updated_ref.at[:, part(t)], keep_sem)

    loads = [
        pltpu.make_async_copy(
            sides_ref.at[t, g, side], keeper.at[:, pl.ds(g * cols + t * WIDTH, WIDTH)],
            side_sem.at[t, g, side],
        )
        for t in range(steps)
        for g in range(ring)
        for side, keeper in enumerate((left, right))
    ]
    for load in loads:
        load.start()
    total_ref[...] = jnp.zeros_like(total_ref)
    for load in loads:
        load.wait()

    def multiply(t):
        @pl.when(t >= 2)
        def _():
            for s in range(1, ring):
                across(t - 2, s).wait_send()

        slot = lax.rem(t, 2)

        def channel(c, carry):
            rights = jnp.concatenate(
                [
                    right[c, pl.ds(pl.multiple_of(g * cols + t * WIDTH, WIDTH), WIDTH), :]
                    for g in range(ring)
                ],
                axis=0,
            )
            found = contract_last(rights, left[c]).astype(jnp.bfloat16)
            for g in range(ring):
                product[slot, g, c] = found[g * WIDTH : (g + 1) * WIDTH]
            return carry

        lax.fori_loop(0, quarter, channel, 0, unroll=UNROLL)
        for s in range(1, ring):
            across(t, s).start()
        across_own(t).start()

    def normalise(t):
        for s in range(1, ring):
            across(t, s).wait_recv()
        across_own(t).wait()
        load = pltpu.make_async_copy(tri_ref.at[t], part_ref, load_sem.at[0])
        load.start()

        @pl.when(t >= 2)
        def _():
            for s in range(1, ring):
                homeward(t - 2, s).wait_send()
            homeward_own(t - 2).wait()

        load.wait()
        for q in range(ring):
            for l in range(wide // LANES):
                stage[l, q * quarter * WIDTH : (q + 1) * quarter * WIDTH, :] = (
                    part_ref[q, :, :, l * LANES : (l + 1) * LANES]
                    .astype(jnp.float32)
                    .reshape(quarter * WIDTH, LANES)
                )
        slot = lax.rem(t, 2)

        def column(j, carry):
            for l in range(wide // LANES):
                values = stage[l, pl.ds(j, hidden, stride=WIDTH), :]
                centered = values - jnp.mean(values, axis=0, keepdims=True)
                variance = jnp.mean(centered * centered, axis=0, keepdims=True)
                scaled = centered * lax.rsqrt(variance + EPS)
                turned = scaled.T.astype(jnp.bfloat16)
                for g in range(ring):
                    low, high = max(g * rows, l * LANES), min((g + 1) * rows, (l + 1) * LANES)
                    if low < high:
                        normed_ref[slot, g, j, low - g * rows : high - g * rows, :] = turned[
                            low - l * LANES : high - l * LANES
                        ]
            return carry

        lax.fori_loop(0, WIDTH, column, 0, unroll=UNROLL)
        for s in range(1, ring):
            homeward(t, s).start()
        homeward_own(t).start()

    def finish(t):
        own_load = pltpu.make_async_copy(pair_ref.at[:, part(t)], pair, load_sem.at[1])
        own_load.start()
        for s in range(1, ring):
            homeward(t, s).wait_recv()

        @pl.when(t >= steps - 2)
        def _():
            homeward_own(t).wait()

        home_load = pltpu.make_async_copy(home_ref.at[:, part(t)], home, load_sem.at[0])
        home_load.start()

        @pl.when(t >= 1)
        def _():
            keep(t - 1).wait()

        own_load.wait()
        home_load.wait()

        def column(j, carry):
            for b in range(ring):
                own = pair[b, j].astype(jnp.float32)
                normed = layer_norm(own).astype(jnp.bfloat16)
                gate = jax.nn.sigmoid(
                    jnp.dot(normed, gate_ref[...], preferred_element_type=jnp.float32)
                )
                back = jnp.dot(home[b, j], out_ref[...], preferred_element_type=jnp.float32)
                live = live_ref[b] * col_ref[b, t * WIDTH + j]
                one = (own + live * gate * back).astype(jnp.bfloat16)
                result[b, j] = one
                size = jnp.abs(one.astype(jnp.float32)).reshape(rows // 8, 8, channels)
                total_ref[...] += jnp.sum(size, axis=0)
            return carry

        lax.fori_loop(0, WIDTH, column, 0, unroll=UNROLL)
        keep(t).start()

    lag = 3

    def step(t, carry):
        @pl.when(t < steps)
        def _():
            multiply(t)

        @pl.when(jnp.logical_and(t >= 1, t < steps + 1))
        def _():
            normalise(t - 1)

        @pl.when(t >= lag)
        def _():
            finish(t - lag)

        return carry

    lax.fori_loop(0, steps + lag, step, 0)
    sending = []
    for phase, (axis, size) in enumerate(axes):
        here = lax.axis_index(axis)
        sums[phase] = total_ref[...]
        boxes[phase, here] = total_ref[...]
        copies = [
            remote(
                sums.at[phase], boxes.at[phase, here], sum_send.at[phase, s - 1],
                sum_recv.at[phase, s - 1], axis, lax.rem(here + s, size),
            )
            for s in range(1, size)
        ]
        for copy in copies:
            copy.start()
        for copy in copies:
            copy.wait_recv()
        total_ref[...] = jnp.sum(boxes[phase, :size], axis=0)
        sending += copies
    for copy in sending:
        copy.wait_send()
    keep(steps - 1).wait()
    for t in range(max(steps - 2, 0), steps):
        for s in range(1, ring):
            across(t, s).wait_send()
            homeward(t, s).wait_send()


def rehomed(pair_repr, seq_lengths, weight_in, weight_out):
    ring, rows, cols, channels = pair_repr.shape
    hidden = weight_out.shape[0]
    quarter = hidden // ring
    steps = cols // WIDTH
    deep = ring * rows
    pairs = lax.axis_size("gz")
    most = max(ring, pairs)
    me = lax.axis_index("gx")
    row_first = me * rows
    col_first = lax.axis_index("gy") * cols
    lengths = lax.dynamic_slice_in_dim(seq_lengths, lax.axis_index("gz") * ring, ring)
    length = lax.dynamic_index_in_dim(lengths, me, 0, keepdims=False)
    row_local = jnp.arange(rows, dtype=jnp.int32)
    col_at = col_first + jnp.arange(cols, dtype=jnp.int32)
    k_at = jnp.concatenate([jnp.bitwise_xor(me, s) * rows + row_local for s in range(ring)])
    mask = ((col_at < length)[:, None] & (k_at < length)[None, :]).astype(jnp.float32)
    row_live = ((row_first + row_local)[None, :] < lengths[:, None]).astype(jnp.float32)
    row_live = jnp.broadcast_to(row_live[:, :, None], (ring, rows, channels))
    col_live = (col_at[None, :] < lengths[:, None]).astype(jnp.float32)
    pair_t = pair_repr.transpose(0, 2, 1, 3)
    weight_t = weight_in[:, : 4 * hidden].T
    any_space = pl.BlockSpec(memory_space=pl.ANY)
    vmem = pl.BlockSpec(memory_space=pltpu.VMEM)
    smem = pl.BlockSpec(memory_space=pltpu.SMEM)
    dma = pltpu.SemaphoreType.DMA
    f32, bf16 = jnp.float32, jnp.bfloat16

    sides, _ = pl.pallas_call(
        functools.partial(enter_kernel, ring),
        out_shape=(
            jax.ShapeDtypeStruct((steps, ring, 2, quarter, WIDTH, deep), bf16),
            jax.ShapeDtypeStruct((ring - 1, cols, rows, channels), bf16),
        ),
        in_specs=[any_space, vmem, vmem],
        out_specs=(any_space, any_space),
        scratch_shapes=[
            pltpu.VMEM((WIDTH, deep, channels), bf16),
            pltpu.VMEM((deep // LANES, 2 * hidden * WIDTH, LANES), f32),
            pltpu.VMEM((2, ring, 2, quarter, WIDTH, deep), bf16),
            dma((ring,)),
            dma((steps, ring - 1)),
            dma((steps, ring - 1)),
            dma((steps, ring - 1)),
            dma((steps, ring - 1)),
            dma((steps,)),
        ],
        compiler_params=pltpu.CompilerParams(
            collective_id=0, has_side_effects=True, vmem_limit_bytes=60 * 1024 * 1024
        ),
        name="enter",
    )(pair_t, weight_t, mask)

    updated_t, total, _, _ = pl.pallas_call(
        functools.partial(leave_kernel, ring, pairs),
        out_shape=(
            jax.ShapeDtypeStruct(pair_t.shape, bf16),
            jax.ShapeDtypeStruct((8, channels), f32),
            jax.ShapeDtypeStruct((steps, ring, quarter, WIDTH, ring * rows), bf16),
            jax.ShapeDtypeStruct((ring, cols, rows, channels), bf16),
        ),
        in_specs=[any_space, any_space, vmem, vmem, vmem, smem],
        out_specs=(any_space, vmem, any_space, any_space),
        scratch_shapes=[
            pltpu.VMEM((quarter, ring * cols, deep), bf16),
            pltpu.VMEM((quarter, ring * cols, deep), bf16),
            pltpu.VMEM((2, ring, quarter, WIDTH, ring * rows), bf16),
            pltpu.VMEM((ring, quarter, WIDTH, ring * rows), bf16),
            pltpu.VMEM((ring * rows // LANES, hidden * WIDTH, LANES), f32),
            pltpu.VMEM((2, ring, WIDTH, rows, channels), bf16),
            pltpu.VMEM((ring, WIDTH, rows, channels), bf16),
            pltpu.VMEM((ring, WIDTH, rows, channels), bf16),
            pltpu.VMEM((ring, WIDTH, rows, channels), bf16),
            pltpu.VMEM((3, 8, channels), f32),
            pltpu.VMEM((3, most, 8, channels), f32),
            dma((2,)),
            dma((steps, ring - 1)),
            dma((steps, ring - 1)),
            dma((steps,)),
            dma((steps, ring - 1)),
            dma((steps, ring - 1)),
            dma((steps,)),
            dma(()),
            dma((3, most - 1)),
            dma((3, most - 1)),
            dma((steps, ring, 2)),
        ],
        compiler_params=pltpu.CompilerParams(
            collective_id=1, has_side_effects=True, vmem_limit_bytes=60 * 1024 * 1024
        ),
        name="leave",
    )(sides, pair_t, weight_in[:, 4 * hidden :], weight_out, row_live, col_live)

    updated = updated_t.transpose(0, 2, 1, 3)
    entry_count = ring * pairs * rows * ring * cols * lax.axis_size("gy") * channels
    return (updated, jnp.sum(total) / float(entry_count))


def gathered_columns(pair_repr, seq_lengths, weight_in, weight_out):
    batch_dev, row_count, col_count, channels = pair_repr.shape
    hidden = weight_out.shape[0]
    row_first = lax.axis_index("gx") * row_count
    col_first = lax.axis_index("gy") * col_count
    my_lengths = lax.dynamic_slice_in_dim(seq_lengths, lax.axis_index("gz") * batch_dev, batch_dev)
    row_at = row_first + jnp.arange(row_count, dtype=jnp.int32)
    col_at = col_first + jnp.arange(col_count, dtype=jnp.int32)

    def gated(normed, first, mask):
        part = weight_in[:, first : first + 2 * hidden]
        proj = jnp.einsum("ijc,cd->ijd", normed, part, preferred_element_type=jnp.float32)
        return (mask * jax.nn.sigmoid(proj[..., hidden:]) * proj[..., :hidden]).astype(
            jnp.bfloat16
        )

    masks, normed, gathered, shares = [], [], [], []
    for b in range(batch_dev):
        row_live = (row_at < my_lengths[b]).astype(jnp.float32)
        col_live = (col_at < my_lengths[b]).astype(jnp.float32)
        masks.append(row_live[:, None, None] * col_live[None, :, None])
        normed.append(layer_norm(pair_repr[b].astype(jnp.float32)).astype(jnp.bfloat16))
        left = gated(normed[b], 0, masks[b])
        gathered.append(lax.all_gather(left, "gy", axis=1, tiled=True))
    for b in range(batch_dev):
        right = gated(normed[b], 2 * hidden, masks[b])
        partial = jnp.einsum(
            "kic,kjc->ijc", gathered[b], right, preferred_element_type=jnp.float32
        ).astype(jnp.bfloat16)
        shares.append(lax.psum_scatter(partial, "gx", scatter_dimension=0, tiled=True))
    outs, total = [], jnp.float32(0)
    for b in range(batch_dev):
        gate_values = jax.nn.sigmoid(
            jnp.einsum(
                "ijc,cd->ijd", normed[b], weight_in[:, 4 * hidden :],
                preferred_element_type=jnp.float32,
            )
        )
        tri_normed = layer_norm(shares[b].astype(jnp.float32)).astype(jnp.bfloat16)
        projected = jnp.einsum(
            "ijc,cd->ijd", tri_normed, weight_out, preferred_element_type=jnp.float32
        )
        update = masks[b] * gate_values * projected
        one = (pair_repr[b].astype(jnp.float32) + update).astype(jnp.bfloat16)
        outs.append(one)
        total = total + jnp.sum(jnp.abs(one.astype(jnp.float32)))
    updated = jnp.stack(outs)
    mag_total = lax.psum(total, ("gz", "gx", "gy"))
    entry_count = (
        batch_dev
        * lax.axis_size("gz")
        * row_count
        * lax.axis_size("gx")
        * col_count
        * lax.axis_size("gy")
        * channels
    )
    magnitude = mag_total / float(entry_count)
    return (updated, magnitude)


def per_device(pair_repr, seq_lengths, weight_in, weight_out):
    ring, rows, cols, channels = pair_repr.shape
    square = lax.axis_size("gx") == ring and lax.axis_size("gy") == ring and ring & (ring - 1) == 0
    tiled = rows % WIDTH == 0 and cols % WIDTH == 0 and ring * rows % LANES == 0
    if square and tiled and channels == LANES and weight_out.shape[0] == LANES:
        return rehomed(pair_repr, seq_lengths, weight_in, weight_out)
    return gathered_columns(pair_repr, seq_lengths, weight_in, weight_out)


def solution(mesh):
    return jax.shard_map(
        per_device,
        mesh=mesh,
        in_specs=(P("gz", "gx", "gy", None), P(), P(), P()),
        out_specs=(P("gz", "gx", "gy", None), P()),
        check_vma=False,
    )
```

```python
import functools

import jax
import jax.numpy as jnp
from jax import lax
from jax.experimental import pallas as pl
from jax.experimental.pallas import tpu as pltpu
from jax.sharding import PartitionSpec as P

WIDTH = 16
UNROLL = 2
WINDOW = 1
LANES = 128
EPS = 1e-05


def layer_norm(values):
    mean_value = jnp.mean(values, axis=-1, keepdims=True)
    centered = values - mean_value
    variance = jnp.mean(centered * centered, axis=-1, keepdims=True)
    return centered * lax.rsqrt(variance + EPS)


def contract_last(a, b):
    return lax.dot_general(a, b, (((1,), (1,)), ((), ())), preferred_element_type=jnp.float32)


def meet(axes):
    barrier = pltpu.get_barrier_semaphore()
    for axis, size in axes:
        me = lax.axis_index(axis)
        for s in range(1, size):
            pl.semaphore_signal(
                barrier, inc=1, device_id={axis: lax.rem(me + s, size)},
                device_id_type=pl.DeviceIdType.MESH,
            )
    pl.semaphore_wait(barrier, sum(size - 1 for _, size in axes))


def remote(src, dst, send, recv, axis, target):
    return pltpu.make_async_remote_copy(
        src_ref=src, dst_ref=dst, send_sem=send, recv_sem=recv,
        device_id={axis: target}, device_id_type=pl.DeviceIdType.MESH,
    )


def whole_kernel(
    ring, pairs, pair_ref, weight_ref, gate_ref, out_ref, mask_ref, live_ref, col_ref,
    updated_ref, total_ref, got_ref, tri_ref, home_ref,
    block, turn, stage, ready, left, right, product, part_ref, normed_ref, home, pair, result,
    sums, boxes,
    load_sem, in_send, in_recv, side_send, side_recv, side_own, y_send, y_recv, y_own,
    z_send, z_recv, z_own, keep_sem, sum_send, sum_recv,
):
    me, col = lax.axis_index("gx"), lax.axis_index("gy")
    rows, cols, channels = pair_ref.shape[1:]
    hidden = weight_ref.shape[0] // 4
    quarter = hidden // ring
    steps = cols // WIDTH
    deep = ring * rows
    wide = ring * rows
    tall = rows * WIDTH
    axes = (("gx", ring), ("gy", ring), ("gz", pairs))
    meet(axes)

    def part(t):
        return pl.ds(pl.multiple_of(t * WIDTH, WIDTH), WIDTH)

    def inbound(t, s):
        target = jnp.bitwise_xor(me, s)
        return remote(
            pair_ref.at[target, :, part(t)], got_ref.at[t, s - 1],
            in_send.at[t, s - 1], in_recv.at[t, s - 1], "gx", target,
        )

    def place(t):
        return pl.ds(pl.multiple_of(col * cols + t * WIDTH, WIDTH), WIDTH)

    def outbound(t, s, side):
        target = jnp.bitwise_xor(col, s)
        return remote(
            ready.at[lax.rem(t, 2), target, side], (left, right)[side].at[:, place(t)],
            side_send.at[t, s - 1, side], side_recv.at[t, s - 1, side], "gy", target,
        )

    for t in range(min(WINDOW, steps)):
        for s in range(1, ring):
            inbound(t, s).start()

    def drain(t):
        for side in range(2):
            for s in range(1, ring):
                outbound(t, s, side).wait_send()

    def gather(t, carry):
        for s in range(1, ring):
            inbound(t, s).wait_recv()

        @pl.when(t + WINDOW < steps)
        def _():
            for s in range(1, ring):
                inbound(t + WINDOW, s).start()

        loads = []
        for s in range(ring):
            src = pair_ref.at[me, :, part(t)] if s == 0 else got_ref.at[t, s - 1]
            loads.append(
                pltpu.make_async_copy(src, block.at[pl.ds(s * rows, rows)], load_sem.at[s])
            )
            loads[-1].start()
        for s in range(ring):
            loads[s].wait()
            turn[s * tall : (s + 1) * tall, :] = (
                block[s * rows : (s + 1) * rows].astype(jnp.float32).reshape(tall, channels)
            )

        def column(i, carry):
            normed = layer_norm(turn[pl.ds(i, deep, stride=WIDTH), :]).astype(jnp.bfloat16)
            proj = contract_last(weight_ref[...], normed)
            live = mask_ref[pl.ds(t * WIDTH + i, 1), :]
            for side in range(2):
                first = 2 * side * hidden
                value = proj[first : first + hidden]
                gate = proj[first + hidden : first + 2 * hidden]
                out = live * jax.nn.sigmoid(gate) * value
                for l in range(deep // LANES):
                    stage[l, pl.ds(side * hidden * WIDTH + i, hidden, stride=WIDTH), :] = out[
                        :, l * LANES : (l + 1) * LANES
                    ]
            return carry

        lax.fori_loop(0, WIDTH, column, 0, unroll=UNROLL)

        @pl.when(t >= 2)
        def _():
            drain(t - 2)

        slot = lax.rem(t, 2)
        for side in range(2):
            for q in range(ring):
                first = (side * hidden + q * quarter) * WIDTH
                for l in range(deep // LANES):
                    ready[slot, q, side, :, :, l * LANES : (l + 1) * LANES] = (
                        stage[l, first : first + quarter * WIDTH, :]
                        .reshape(quarter, WIDTH, LANES)
                        .astype(jnp.bfloat16)
                    )
            for s in range(1, ring):
                outbound(t, s, side).start()
            (left, right)[side][:, place(t)] = ready[slot, col, side]
        return carry

    lax.fori_loop(0, steps, gather, 0)

    def across(t, s):
        target = jnp.bitwise_xor(col, s)
        return remote(
            product.at[lax.rem(t, 2), target], tri_ref.at[t, col],
            y_send.at[t, s - 1], y_recv.at[t, s - 1], "gy", target,
        )

    def across_own(t):
        return pltpu.make_async_copy(
            product.at[lax.rem(t, 2), col], tri_ref.at[t, col], y_own.at[t]
        )

    def homeward(t, s):
        target = jnp.bitwise_xor(me, s)
        return remote(
            normed_ref.at[lax.rem(t, 2), target], home_ref.at[me, part(t)],
            z_send.at[t, s - 1], z_recv.at[t, s - 1], "gx", target,
        )

    def homeward_own(t):
        return pltpu.make_async_copy(
            normed_ref.at[lax.rem(t, 2), me], home_ref.at[me, part(t)], z_own.at[t]
        )

    def keep(t):
        return pltpu.make_async_copy(result, updated_ref.at[:, :, part(t)], keep_sem)

    total_ref[...] = jnp.zeros_like(total_ref)
    for t in range(steps):
        for s in range(1, ring):
            outbound(t, s, 0).wait_recv()

    def multiply(t):
        for s in range(1, ring):
            outbound(t, s, 1).wait_recv()

        @pl.when(t >= 2)
        def _():
            for s in range(1, ring):
                across(t - 2, s).wait_send()

        slot = lax.rem(t, 2)

        def channel(c, carry):
            rights = jnp.concatenate(
                [
                    right[c, pl.ds(pl.multiple_of(g * cols + t * WIDTH, WIDTH), WIDTH), :]
                    for g in range(ring)
                ],
                axis=0,
            )
            found = contract_last(rights, left[c]).astype(jnp.bfloat16)
            for g in range(ring):
                product[slot, g, c] = found[g * WIDTH : (g + 1) * WIDTH]
            return carry

        lax.fori_loop(0, quarter, channel, 0, unroll=UNROLL)
        for s in range(1, ring):
            across(t, s).start()
        across_own(t).start()

    def normalise(t):
        for s in range(1, ring):
            across(t, s).wait_recv()
        across_own(t).wait()
        load = pltpu.make_async_copy(tri_ref.at[t], part_ref, load_sem.at[0])
        load.start()

        @pl.when(t >= 2)
        def _():
            for s in range(1, ring):
                homeward(t - 2, s).wait_send()
            homeward_own(t - 2).wait()

        load.wait()
        for q in range(ring):
            for l in range(wide // LANES):
                stage[l, q * quarter * WIDTH : (q + 1) * quarter * WIDTH, :] = (
                    part_ref[q, :, :, l * LANES : (l + 1) * LANES]
                    .astype(jnp.float32)
                    .reshape(quarter * WIDTH, LANES)
                )
        slot = lax.rem(t, 2)

        def column(j, carry):
            for l in range(wide // LANES):
                values = stage[l, pl.ds(j, hidden, stride=WIDTH), :]
                centered = values - jnp.mean(values, axis=0, keepdims=True)
                variance = jnp.mean(centered * centered, axis=0, keepdims=True)
                scaled = centered * lax.rsqrt(variance + EPS)
                turned = scaled.T.astype(jnp.bfloat16)
                for g in range(ring):
                    low, high = max(g * rows, l * LANES), min((g + 1) * rows, (l + 1) * LANES)
                    if low < high:
                        normed_ref[slot, g, j, low - g * rows : high - g * rows, :] = turned[
                            low - l * LANES : high - l * LANES
                        ]
            return carry

        lax.fori_loop(0, WIDTH, column, 0, unroll=UNROLL)
        for s in range(1, ring):
            homeward(t, s).start()
        homeward_own(t).start()

    def finish(t):
        own_load = pltpu.make_async_copy(pair_ref.at[:, :, part(t)], pair, load_sem.at[1])
        own_load.start()
        own_load.wait()
        for b in range(ring):
            turn[b * tall : (b + 1) * tall, :] = (
                pair[b].astype(jnp.float32).reshape(tall, channels)
            )
        for s in range(1, ring):
            homeward(t, s).wait_recv()

        @pl.when(t >= steps - 2)
        def _():
            homeward_own(t).wait()

        home_load = pltpu.make_async_copy(home_ref.at[:, part(t)], home, load_sem.at[0])
        home_load.start()

        @pl.when(t >= 1)
        def _():
            keep(t - 1).wait()

        home_load.wait()

        def column(j, carry):
            for b in range(ring):
                own = turn[pl.ds(b * tall + j, rows, stride=WIDTH), :]
                normed = layer_norm(own).astype(jnp.bfloat16)
                gate = jax.nn.sigmoid(
                    jnp.dot(normed, gate_ref[...], preferred_element_type=jnp.float32)
                )
                back = jnp.dot(home[b, j], out_ref[...], preferred_element_type=jnp.float32)
                live = live_ref[b] * col_ref[b, t * WIDTH + j]
                one = (own + live * gate * back).astype(jnp.bfloat16).astype(jnp.float32)
                turn[pl.ds(b * tall + j, rows, stride=WIDTH), :] = one
                total_ref[...] += jnp.sum(jnp.abs(one).reshape(rows // 8, 8, channels), axis=0)
            return carry

        lax.fori_loop(0, WIDTH, column, 0, unroll=UNROLL)
        for b in range(ring):
            result[b] = (
                turn[b * tall : (b + 1) * tall, :]
                .reshape(rows, WIDTH, channels)
                .astype(jnp.bfloat16)
            )
        keep(t).start()

    lag = 3

    def spread(t, carry):
        @pl.when(t < steps)
        def _():
            multiply(t)

        @pl.when(jnp.logical_and(t >= 1, t < steps + 1))
        def _():
            normalise(t - 1)

        @pl.when(t >= lag)
        def _():
            finish(t - lag)

        return carry

    lax.fori_loop(0, steps + lag, spread, 0)
    sending = []
    for phase, (axis, size) in enumerate(axes):
        here = lax.axis_index(axis)
        sums[phase] = total_ref[...]
        boxes[phase, here] = total_ref[...]
        copies = [
            remote(
                sums.at[phase], boxes.at[phase, here], sum_send.at[phase, s - 1],
                sum_recv.at[phase, s - 1], axis, lax.rem(here + s, size),
            )
            for s in range(1, size)
        ]
        for copy in copies:
            copy.start()
        for copy in copies:
            copy.wait_recv()
        total_ref[...] = jnp.sum(boxes[phase, :size], axis=0)
        sending += copies
    for copy in sending:
        copy.wait_send()
    keep(steps - 1).wait()
    for t in range(max(steps - 2, 0), steps):
        drain(t)
        for s in range(1, ring):
            across(t, s).wait_send()
            homeward(t, s).wait_send()
    for t in range(steps):
        for s in range(1, ring):
            inbound(t, s).wait_send()


def rehomed(pair_repr, seq_lengths, weight_in, weight_out):
    ring, rows, cols, channels = pair_repr.shape
    hidden = weight_out.shape[0]
    quarter = hidden // ring
    steps = cols // WIDTH
    deep = ring * rows
    pairs = lax.axis_size("gz")
    most = max(ring, pairs)
    me = lax.axis_index("gx")
    row_first = me * rows
    col_first = lax.axis_index("gy") * cols
    lengths = lax.dynamic_slice_in_dim(seq_lengths, lax.axis_index("gz") * ring, ring)
    length = lax.dynamic_index_in_dim(lengths, me, 0, keepdims=False)
    row_local = jnp.arange(rows, dtype=jnp.int32)
    col_at = col_first + jnp.arange(cols, dtype=jnp.int32)
    k_at = jnp.concatenate([jnp.bitwise_xor(me, s) * rows + row_local for s in range(ring)])
    mask = ((col_at < length)[:, None] & (k_at < length)[None, :]).astype(jnp.float32)
    row_live = ((row_first + row_local)[None, :] < lengths[:, None]).astype(jnp.float32)
    row_live = jnp.broadcast_to(row_live[:, :, None], (ring, rows, channels))
    col_live = (col_at[None, :] < lengths[:, None]).astype(jnp.float32)
    any_space = pl.BlockSpec(memory_space=pl.ANY)
    vmem = pl.BlockSpec(memory_space=pltpu.VMEM)
    smem = pl.BlockSpec(memory_space=pltpu.SMEM)
    dma = pltpu.SemaphoreType.DMA
    f32, bf16 = jnp.float32, jnp.bfloat16

    updated, total, _, _, _ = pl.pallas_call(
        functools.partial(whole_kernel, ring, pairs),
        out_shape=(
            jax.ShapeDtypeStruct(pair_repr.shape, bf16),
            jax.ShapeDtypeStruct((8, channels), f32),
            jax.ShapeDtypeStruct((steps, ring - 1, rows, WIDTH, channels), bf16),
            jax.ShapeDtypeStruct((steps, ring, quarter, WIDTH, ring * rows), bf16),
            jax.ShapeDtypeStruct((ring, cols, rows, channels), bf16),
        ),
        in_specs=[any_space, vmem, vmem, vmem, vmem, vmem, smem],
        out_specs=(any_space, vmem, any_space, any_space, any_space),
        scratch_shapes=[
            pltpu.VMEM((deep, WIDTH, channels), bf16),
            pltpu.VMEM((deep * WIDTH, channels), f32),
            pltpu.VMEM((deep // LANES, 2 * hidden * WIDTH, LANES), f32),
            pltpu.VMEM((2, ring, 2, quarter, WIDTH, deep), bf16),
            pltpu.VMEM((quarter, ring * cols, deep), bf16),
            pltpu.VMEM((quarter, ring * cols, deep), bf16),
            pltpu.VMEM((2, ring, quarter, WIDTH, ring * rows), bf16),
            pltpu.VMEM((ring, quarter, WIDTH, ring * rows), bf16),
            pltpu.VMEM((2, ring, WIDTH, rows, channels), bf16),
            pltpu.VMEM((ring, WIDTH, rows, channels), bf16),
            pltpu.VMEM((ring, rows, WIDTH, channels), bf16),
            pltpu.VMEM((ring, rows, WIDTH, channels), bf16),
            pltpu.VMEM((3, 8, channels), f32),
            pltpu.VMEM((3, most, 8, channels), f32),
            dma((ring,)),
            dma((steps, ring - 1)),
            dma((steps, ring - 1)),
            dma((steps, ring - 1, 2)),
            dma((steps, ring - 1, 2)),
            dma((steps, 2)),
            dma((steps, ring - 1)),
            dma((steps, ring - 1)),
            dma((steps,)),
            dma((steps, ring - 1)),
            dma((steps, ring - 1)),
            dma((steps,)),
            dma(()),
            dma((3, most - 1)),
            dma((3, most - 1)),
        ],
        compiler_params=pltpu.CompilerParams(
            collective_id=0, has_side_effects=True, vmem_limit_bytes=60 * 1024 * 1024
        ),
        name="whole",
    )(pair_repr, weight_in[:, : 4 * hidden].T, weight_in[:, 4 * hidden :], weight_out, mask, row_live, col_live)
    entry_count = ring * pairs * rows * ring * cols * lax.axis_size("gy") * channels
    return (updated, jnp.sum(total) / float(entry_count))


def gathered_columns(pair_repr, seq_lengths, weight_in, weight_out):
    batch_dev, row_count, col_count, channels = pair_repr.shape
    hidden = weight_out.shape[0]
    row_first = lax.axis_index("gx") * row_count
    col_first = lax.axis_index("gy") * col_count
    my_lengths = lax.dynamic_slice_in_dim(seq_lengths, lax.axis_index("gz") * batch_dev, batch_dev)
    row_at = row_first + jnp.arange(row_count, dtype=jnp.int32)
    col_at = col_first + jnp.arange(col_count, dtype=jnp.int32)

    def gated(normed, first, mask):
        part = weight_in[:, first : first + 2 * hidden]
        proj = jnp.einsum("ijc,cd->ijd", normed, part, preferred_element_type=jnp.float32)
        return (mask * jax.nn.sigmoid(proj[..., hidden:]) * proj[..., :hidden]).astype(
            jnp.bfloat16
        )

    masks, normed, gathered, shares = [], [], [], []
    for b in range(batch_dev):
        row_live = (row_at < my_lengths[b]).astype(jnp.float32)
        col_live = (col_at < my_lengths[b]).astype(jnp.float32)
        masks.append(row_live[:, None, None] * col_live[None, :, None])
        normed.append(layer_norm(pair_repr[b].astype(jnp.float32)).astype(jnp.bfloat16))
        left = gated(normed[b], 0, masks[b])
        gathered.append(lax.all_gather(left, "gy", axis=1, tiled=True))
    for b in range(batch_dev):
        right = gated(normed[b], 2 * hidden, masks[b])
        partial = jnp.einsum(
            "kic,kjc->ijc", gathered[b], right, preferred_element_type=jnp.float32
        ).astype(jnp.bfloat16)
        shares.append(lax.psum_scatter(partial, "gx", scatter_dimension=0, tiled=True))
    outs, total = [], jnp.float32(0)
    for b in range(batch_dev):
        gate_values = jax.nn.sigmoid(
            jnp.einsum(
                "ijc,cd->ijd", normed[b], weight_in[:, 4 * hidden :],
                preferred_element_type=jnp.float32,
            )
        )
        tri_normed = layer_norm(shares[b].astype(jnp.float32)).astype(jnp.bfloat16)
        projected = jnp.einsum(
            "ijc,cd->ijd", tri_normed, weight_out, preferred_element_type=jnp.float32
        )
        update = masks[b] * gate_values * projected
        one = (pair_repr[b].astype(jnp.float32) + update).astype(jnp.bfloat16)
        outs.append(one)
        total = total + jnp.sum(jnp.abs(one.astype(jnp.float32)))
    updated = jnp.stack(outs)
    mag_total = lax.psum(total, ("gz", "gx", "gy"))
    entry_count = (
        batch_dev
        * lax.axis_size("gz")
        * row_count
        * lax.axis_size("gx")
        * col_count
        * lax.axis_size("gy")
        * channels
    )
    magnitude = mag_total / float(entry_count)
    return (updated, magnitude)


def per_device(pair_repr, seq_lengths, weight_in, weight_out):
    ring, rows, cols, channels = pair_repr.shape
    square = lax.axis_size("gx") == ring and lax.axis_size("gy") == ring and ring & (ring - 1) == 0
    tiled = rows % WIDTH == 0 and cols % WIDTH == 0 and ring * rows % LANES == 0
    if square and tiled and channels == LANES and weight_out.shape[0] == LANES:
        return rehomed(pair_repr, seq_lengths, weight_in, weight_out)
    return gathered_columns(pair_repr, seq_lengths, weight_in, weight_out)


def solution(mesh):
    return jax.shard_map(
        per_device,
        mesh=mesh,
        in_specs=(P("gz", "gx", "gy", None), P(), P(), P()),
        out_specs=(P("gz", "gx", "gy", None), P()),
        check_vma=False,
    )
```

```python
import functools

import jax
import jax.numpy as jnp
from jax import lax
from jax.experimental import pallas as pl
from jax.experimental.pallas import tpu as pltpu
from jax.sharding import PartitionSpec as P

WIDTH = 16
UNROLL = 2
WINDOW = 1
AHEAD = 2
LANES = 128
EPS = 1e-05


def layer_norm(values):
    mean_value = jnp.mean(values, axis=-1, keepdims=True)
    centered = values - mean_value
    variance = jnp.mean(centered * centered, axis=-1, keepdims=True)
    return centered * lax.rsqrt(variance + EPS)


def contract_last(a, b):
    return lax.dot_general(a, b, (((1,), (1,)), ((), ())), preferred_element_type=jnp.float32)


def meet(axes):
    barrier = pltpu.get_barrier_semaphore()
    for axis, size in axes:
        me = lax.axis_index(axis)
        for s in range(1, size):
            pl.semaphore_signal(
                barrier, inc=1, device_id={axis: lax.rem(me + s, size)},
                device_id_type=pl.DeviceIdType.MESH,
            )
    pl.semaphore_wait(barrier, sum(size - 1 for _, size in axes))


def remote(src, dst, send, recv, axis, target):
    return pltpu.make_async_remote_copy(
        src_ref=src, dst_ref=dst, send_sem=send, recv_sem=recv,
        device_id={axis: target}, device_id_type=pl.DeviceIdType.MESH,
    )


def whole_kernel(
    ring, pairs, pair_ref, weight_ref, gate_ref, out_ref, mask_ref, live_ref, col_ref,
    updated_ref, total_ref, got_ref, tri_ref, home_ref,
    block, turn, stage, ready, left, right, product, part_ref, normed_ref, home, pair, result,
    sums, boxes,
    load_sem, in_send, in_recv, side_send, side_recv, side_own, y_send, y_recv, y_own,
    z_send, z_recv, z_own, keep_sem, sum_send, sum_recv,
):
    me, col = lax.axis_index("gx"), lax.axis_index("gy")
    rows, cols, channels = pair_ref.shape[1:]
    hidden = weight_ref.shape[0] // 4
    quarter = hidden // ring
    steps = cols // WIDTH
    deep = ring * rows
    wide = ring * rows
    tall = rows * WIDTH
    axes = (("gx", ring), ("gy", ring), ("gz", pairs))
    meet(axes)

    def part(t):
        return pl.ds(pl.multiple_of(t * WIDTH, WIDTH), WIDTH)

    def inbound(t, s):
        target = jnp.bitwise_xor(me, s)
        return remote(
            pair_ref.at[target, :, part(t)], got_ref.at[t, s - 1],
            in_send.at[t, s - 1], in_recv.at[t, s - 1], "gx", target,
        )

    def place(t):
        return pl.ds(pl.multiple_of(col * cols + t * WIDTH, WIDTH), WIDTH)

    def outbound(t, s, side):
        target = jnp.bitwise_xor(col, s)
        return remote(
            ready.at[lax.rem(t, 2), target, side], (left, right)[side].at[:, place(t)],
            side_send.at[t, s - 1, side], side_recv.at[t, s - 1, side], "gy", target,
        )

    inner = jnp.logical_and(me > 0, me < ring - 1)
    for t in range(min(WINDOW, steps)):
        for s in range(1, ring):
            inbound(t, s).start()

    @pl.when(inner)
    def _():
        for t in range(WINDOW, min(AHEAD, steps)):
            for s in range(1, ring):
                inbound(t, s).start()

    def drain(t):
        for side in range(2):
            for s in range(1, ring):
                outbound(t, s, side).wait_send()

    def gather(t, carry):
        for s in range(1, ring):
            inbound(t, s).wait_recv()

        for apart, window in ((inner, AHEAD), (jnp.logical_not(inner), WINDOW)):

            @pl.when(jnp.logical_and(apart, t + window < steps))
            def _():
                for s in range(1, ring):
                    inbound(t + window, s).start()

        loads = []
        for s in range(ring):
            src = pair_ref.at[me, :, part(t)] if s == 0 else got_ref.at[t, s - 1]
            loads.append(
                pltpu.make_async_copy(src, block.at[pl.ds(s * rows, rows)], load_sem.at[s])
            )
            loads[-1].start()
        for s in range(ring):
            loads[s].wait()
            turn[s * tall : (s + 1) * tall, :] = (
                block[s * rows : (s + 1) * rows].astype(jnp.float32).reshape(tall, channels)
            )

        def column(i, carry):
            normed = layer_norm(turn[pl.ds(i, deep, stride=WIDTH), :]).astype(jnp.bfloat16)
            proj = contract_last(weight_ref[...], normed)
            live = mask_ref[pl.ds(t * WIDTH + i, 1), :]
            for side in range(2):
                first = 2 * side * hidden
                value = proj[first : first + hidden]
                gate = proj[first + hidden : first + 2 * hidden]
                out = live * jax.nn.sigmoid(gate) * value
                for l in range(deep // LANES):
                    stage[l, pl.ds(side * hidden * WIDTH + i, hidden, stride=WIDTH), :] = out[
                        :, l * LANES : (l + 1) * LANES
                    ]
            return carry

        lax.fori_loop(0, WIDTH, column, 0, unroll=UNROLL)

        @pl.when(t >= 2)
        def _():
            drain(t - 2)

        slot = lax.rem(t, 2)
        for side in range(2):
            for q in range(ring):
                first = (side * hidden + q * quarter) * WIDTH
                for l in range(deep // LANES):
                    ready[slot, q, side, :, :, l * LANES : (l + 1) * LANES] = (
                        stage[l, first : first + quarter * WIDTH, :]
                        .reshape(quarter, WIDTH, LANES)
                        .astype(jnp.bfloat16)
                    )
            for s in range(1, ring):
                outbound(t, s, side).start()
            (left, right)[side][:, place(t)] = ready[slot, col, side]
        return carry

    lax.fori_loop(0, steps, gather, 0)

    def across(t, s):
        target = jnp.bitwise_xor(col, s)
        return remote(
            product.at[lax.rem(t, 2), target], tri_ref.at[t, col],
            y_send.at[t, s - 1], y_recv.at[t, s - 1], "gy", target,
        )

    def across_own(t):
        return pltpu.make_async_copy(
            product.at[lax.rem(t, 2), col], tri_ref.at[t, col], y_own.at[t]
        )

    def homeward(t, s):
        target = jnp.bitwise_xor(me, s)
        return remote(
            normed_ref.at[lax.rem(t, 2), target], home_ref.at[me, part(t)],
            z_send.at[t, s - 1], z_recv.at[t, s - 1], "gx", target,
        )

    def homeward_own(t):
        return pltpu.make_async_copy(
            normed_ref.at[lax.rem(t, 2), me], home_ref.at[me, part(t)], z_own.at[t]
        )

    def keep(t):
        return pltpu.make_async_copy(result, updated_ref.at[:, :, part(t)], keep_sem)

    total_ref[...] = jnp.zeros_like(total_ref)
    for t in range(steps):
        for s in range(1, ring):
            outbound(t, s, 0).wait_recv()

    def multiply(t):
        for s in range(1, ring):
            outbound(t, s, 1).wait_recv()

        @pl.when(t >= 2)
        def _():
            for s in range(1, ring):
                across(t - 2, s).wait_send()

        slot = lax.rem(t, 2)

        def channel(c, carry):
            rights = jnp.concatenate(
                [
                    right[c, pl.ds(pl.multiple_of(g * cols + t * WIDTH, WIDTH), WIDTH), :]
                    for g in range(ring)
                ],
                axis=0,
            )
            found = contract_last(rights, left[c]).astype(jnp.bfloat16)
            for g in range(ring):
                product[slot, g, c] = found[g * WIDTH : (g + 1) * WIDTH]
            return carry

        lax.fori_loop(0, quarter, channel, 0, unroll=UNROLL)
        for s in range(1, ring):
            across(t, s).start()
        across_own(t).start()

    def normalise(t):
        for s in range(1, ring):
            across(t, s).wait_recv()
        across_own(t).wait()
        load = pltpu.make_async_copy(tri_ref.at[t], part_ref, load_sem.at[0])
        load.start()

        @pl.when(t >= 2)
        def _():
            for s in range(1, ring):
                homeward(t - 2, s).wait_send()
            homeward_own(t - 2).wait()

        load.wait()
        for q in range(ring):
            for l in range(wide // LANES):
                stage[l, q * quarter * WIDTH : (q + 1) * quarter * WIDTH, :] = (
                    part_ref[q, :, :, l * LANES : (l + 1) * LANES]
                    .astype(jnp.float32)
                    .reshape(quarter * WIDTH, LANES)
                )
        slot = lax.rem(t, 2)

        def column(j, carry):
            for l in range(wide // LANES):
                values = stage[l, pl.ds(j, hidden, stride=WIDTH), :]
                centered = values - jnp.mean(values, axis=0, keepdims=True)
                variance = jnp.mean(centered * centered, axis=0, keepdims=True)
                scaled = centered * lax.rsqrt(variance + EPS)
                turned = scaled.T.astype(jnp.bfloat16)
                for g in range(ring):
                    low, high = max(g * rows, l * LANES), min((g + 1) * rows, (l + 1) * LANES)
                    if low < high:
                        normed_ref[slot, g, j, low - g * rows : high - g * rows, :] = turned[
                            low - l * LANES : high - l * LANES
                        ]
            return carry

        lax.fori_loop(0, WIDTH, column, 0, unroll=UNROLL)
        for s in range(1, ring):
            homeward(t, s).start()
        homeward_own(t).start()

    def finish(t):
        own_load = pltpu.make_async_copy(pair_ref.at[:, :, part(t)], pair, load_sem.at[1])
        own_load.start()
        own_load.wait()
        for b in range(ring):
            turn[b * tall : (b + 1) * tall, :] = (
                pair[b].astype(jnp.float32).reshape(tall, channels)
            )
        for s in range(1, ring):
            homeward(t, s).wait_recv()

        @pl.when(t >= steps - 2)
        def _():
            homeward_own(t).wait()

        home_load = pltpu.make_async_copy(home_ref.at[:, part(t)], home, load_sem.at[0])
        home_load.start()

        @pl.when(t >= 1)
        def _():
            keep(t - 1).wait()

        home_load.wait()

        def column(j, carry):
            for b in range(ring):
                own = turn[pl.ds(b * tall + j, rows, stride=WIDTH), :]
                normed = layer_norm(own).astype(jnp.bfloat16)
                gate = jax.nn.sigmoid(
                    jnp.dot(normed, gate_ref[...], preferred_element_type=jnp.float32)
                )
                back = jnp.dot(home[b, j], out_ref[...], preferred_element_type=jnp.float32)
                live = live_ref[b] * col_ref[b, t * WIDTH + j]
                one = (own + live * gate * back).astype(jnp.bfloat16).astype(jnp.float32)
                turn[pl.ds(b * tall + j, rows, stride=WIDTH), :] = one
                total_ref[...] += jnp.sum(jnp.abs(one).reshape(rows // 8, 8, channels), axis=0)
            return carry

        lax.fori_loop(0, WIDTH, column, 0, unroll=UNROLL)
        for b in range(ring):
            result[b] = (
                turn[b * tall : (b + 1) * tall, :]
                .reshape(rows, WIDTH, channels)
                .astype(jnp.bfloat16)
            )
        keep(t).start()

    lag = 3

    def spread(t, carry):
        @pl.when(t < steps)
        def _():
            multiply(t)

        @pl.when(jnp.logical_and(t >= 1, t < steps + 1))
        def _():
            normalise(t - 1)

        @pl.when(t >= lag)
        def _():
            finish(t - lag)

        return carry

    lax.fori_loop(0, steps + lag, spread, 0)
    sending = []
    for phase, (axis, size) in enumerate(axes):
        here = lax.axis_index(axis)
        sums[phase] = total_ref[...]
        boxes[phase, here] = total_ref[...]
        copies = [
            remote(
                sums.at[phase], boxes.at[phase, here], sum_send.at[phase, s - 1],
                sum_recv.at[phase, s - 1], axis, lax.rem(here + s, size),
            )
            for s in range(1, size)
        ]
        for copy in copies:
            copy.start()
        for copy in copies:
            copy.wait_recv()
        total_ref[...] = jnp.sum(boxes[phase, :size], axis=0)
        sending += copies
    for copy in sending:
        copy.wait_send()
    keep(steps - 1).wait()
    for t in range(max(steps - 2, 0), steps):
        drain(t)
        for s in range(1, ring):
            across(t, s).wait_send()
            homeward(t, s).wait_send()
    for t in range(steps):
        for s in range(1, ring):
            inbound(t, s).wait_send()


def rehomed(pair_repr, seq_lengths, weight_in, weight_out):
    ring, rows, cols, channels = pair_repr.shape
    hidden = weight_out.shape[0]
    quarter = hidden // ring
    steps = cols // WIDTH
    deep = ring * rows
    pairs = lax.axis_size("gz")
    most = max(ring, pairs)
    me = lax.axis_index("gx")
    row_first = me * rows
    col_first = lax.axis_index("gy") * cols
    lengths = lax.dynamic_slice_in_dim(seq_lengths, lax.axis_index("gz") * ring, ring)
    length = lax.dynamic_index_in_dim(lengths, me, 0, keepdims=False)
    row_local = jnp.arange(rows, dtype=jnp.int32)
    col_at = col_first + jnp.arange(cols, dtype=jnp.int32)
    k_at = jnp.concatenate([jnp.bitwise_xor(me, s) * rows + row_local for s in range(ring)])
    mask = ((col_at < length)[:, None] & (k_at < length)[None, :]).astype(jnp.float32)
    row_live = ((row_first + row_local)[None, :] < lengths[:, None]).astype(jnp.float32)
    row_live = jnp.broadcast_to(row_live[:, :, None], (ring, rows, channels))
    col_live = (col_at[None, :] < lengths[:, None]).astype(jnp.float32)
    any_space = pl.BlockSpec(memory_space=pl.ANY)
    vmem = pl.BlockSpec(memory_space=pltpu.VMEM)
    smem = pl.BlockSpec(memory_space=pltpu.SMEM)
    dma = pltpu.SemaphoreType.DMA
    f32, bf16 = jnp.float32, jnp.bfloat16

    updated, total, _, _, _ = pl.pallas_call(
        functools.partial(whole_kernel, ring, pairs),
        out_shape=(
            jax.ShapeDtypeStruct(pair_repr.shape, bf16),
            jax.ShapeDtypeStruct((8, channels), f32),
            jax.ShapeDtypeStruct((steps, ring - 1, rows, WIDTH, channels), bf16),
            jax.ShapeDtypeStruct((steps, ring, quarter, WIDTH, ring * rows), bf16),
            jax.ShapeDtypeStruct((ring, cols, rows, channels), bf16),
        ),
        in_specs=[any_space, vmem, vmem, vmem, vmem, vmem, smem],
        out_specs=(any_space, vmem, any_space, any_space, any_space),
        scratch_shapes=[
            pltpu.VMEM((deep, WIDTH, channels), bf16),
            pltpu.VMEM((deep * WIDTH, channels), f32),
            pltpu.VMEM((deep // LANES, 2 * hidden * WIDTH, LANES), f32),
            pltpu.VMEM((2, ring, 2, quarter, WIDTH, deep), bf16),
            pltpu.VMEM((quarter, ring * cols, deep), bf16),
            pltpu.VMEM((quarter, ring * cols, deep), bf16),
            pltpu.VMEM((2, ring, quarter, WIDTH, ring * rows), bf16),
            pltpu.VMEM((ring, quarter, WIDTH, ring * rows), bf16),
            pltpu.VMEM((2, ring, WIDTH, rows, channels), bf16),
            pltpu.VMEM((ring, WIDTH, rows, channels), bf16),
            pltpu.VMEM((ring, rows, WIDTH, channels), bf16),
            pltpu.VMEM((ring, rows, WIDTH, channels), bf16),
            pltpu.VMEM((3, 8, channels), f32),
            pltpu.VMEM((3, most, 8, channels), f32),
            dma((ring,)),
            dma((steps, ring - 1)),
            dma((steps, ring - 1)),
            dma((steps, ring - 1, 2)),
            dma((steps, ring - 1, 2)),
            dma((steps, 2)),
            dma((steps, ring - 1)),
            dma((steps, ring - 1)),
            dma((steps,)),
            dma((steps, ring - 1)),
            dma((steps, ring - 1)),
            dma((steps,)),
            dma(()),
            dma((3, most - 1)),
            dma((3, most - 1)),
        ],
        compiler_params=pltpu.CompilerParams(
            collective_id=0, has_side_effects=True, vmem_limit_bytes=60 * 1024 * 1024
        ),
        name="whole",
    )(pair_repr, weight_in[:, : 4 * hidden].T, weight_in[:, 4 * hidden :], weight_out, mask, row_live, col_live)
    entry_count = ring * pairs * rows * ring * cols * lax.axis_size("gy") * channels
    return (updated, jnp.sum(total) / float(entry_count))


def gathered_columns(pair_repr, seq_lengths, weight_in, weight_out):
    batch_dev, row_count, col_count, channels = pair_repr.shape
    hidden = weight_out.shape[0]
    row_first = lax.axis_index("gx") * row_count
    col_first = lax.axis_index("gy") * col_count
    my_lengths = lax.dynamic_slice_in_dim(seq_lengths, lax.axis_index("gz") * batch_dev, batch_dev)
    row_at = row_first + jnp.arange(row_count, dtype=jnp.int32)
    col_at = col_first + jnp.arange(col_count, dtype=jnp.int32)

    def gated(normed, first, mask):
        part = weight_in[:, first : first + 2 * hidden]
        proj = jnp.einsum("ijc,cd->ijd", normed, part, preferred_element_type=jnp.float32)
        return (mask * jax.nn.sigmoid(proj[..., hidden:]) * proj[..., :hidden]).astype(
            jnp.bfloat16
        )

    masks, normed, gathered, shares = [], [], [], []
    for b in range(batch_dev):
        row_live = (row_at < my_lengths[b]).astype(jnp.float32)
        col_live = (col_at < my_lengths[b]).astype(jnp.float32)
        masks.append(row_live[:, None, None] * col_live[None, :, None])
        normed.append(layer_norm(pair_repr[b].astype(jnp.float32)).astype(jnp.bfloat16))
        left = gated(normed[b], 0, masks[b])
        gathered.append(lax.all_gather(left, "gy", axis=1, tiled=True))
    for b in range(batch_dev):
        right = gated(normed[b], 2 * hidden, masks[b])
        partial = jnp.einsum(
            "kic,kjc->ijc", gathered[b], right, preferred_element_type=jnp.float32
        ).astype(jnp.bfloat16)
        shares.append(lax.psum_scatter(partial, "gx", scatter_dimension=0, tiled=True))
    outs, total = [], jnp.float32(0)
    for b in range(batch_dev):
        gate_values = jax.nn.sigmoid(
            jnp.einsum(
                "ijc,cd->ijd", normed[b], weight_in[:, 4 * hidden :],
                preferred_element_type=jnp.float32,
            )
        )
        tri_normed = layer_norm(shares[b].astype(jnp.float32)).astype(jnp.bfloat16)
        projected = jnp.einsum(
            "ijc,cd->ijd", tri_normed, weight_out, preferred_element_type=jnp.float32
        )
        update = masks[b] * gate_values * projected
        one = (pair_repr[b].astype(jnp.float32) + update).astype(jnp.bfloat16)
        outs.append(one)
        total = total + jnp.sum(jnp.abs(one.astype(jnp.float32)))
    updated = jnp.stack(outs)
    mag_total = lax.psum(total, ("gz", "gx", "gy"))
    entry_count = (
        batch_dev
        * lax.axis_size("gz")
        * row_count
        * lax.axis_size("gx")
        * col_count
        * lax.axis_size("gy")
        * channels
    )
    magnitude = mag_total / float(entry_count)
    return (updated, magnitude)


def per_device(pair_repr, seq_lengths, weight_in, weight_out):
    ring, rows, cols, channels = pair_repr.shape
    square = lax.axis_size("gx") == ring and lax.axis_size("gy") == ring and ring & (ring - 1) == 0
    tiled = rows % WIDTH == 0 and cols % WIDTH == 0 and ring * rows % LANES == 0
    if square and tiled and channels == LANES and weight_out.shape[0] == LANES:
        return rehomed(pair_repr, seq_lengths, weight_in, weight_out)
    return gathered_columns(pair_repr, seq_lengths, weight_in, weight_out)


def solution(mesh):
    return jax.shard_map(
        per_device,
        mesh=mesh,
        in_specs=(P("gz", "gx", "gy", None), P(), P(), P()),
        out_specs=(P("gz", "gx", "gy", None), P()),
        check_vma=False,
    )
```
